32 devices in a mesh: dp: 8 (over z, core), tensor: 4 (over y, x).
Axes of the slice: x: 2, y: 2, z: 4, core: 2. Of those that a mesh axis runs over, the one named last changes fastest.
Arguments:
- tokens: bfloat16 [10240, 4096], P(('dp', 'tensor')), parts along dimension 0, may hold values from -6 to 6
- norm_gain: bfloat16 [4096], replicated, may hold values from 0.099609375 to 1.8984375
- query_weight: bfloat16 [4096, 8192], P(None, 'tensor'), may hold values from -0.09375 to 0.09375
- key_weight: bfloat16 [4096, 1024], P(None, 'tensor'), may hold values from -0.09375 to 0.09375
- value_weight: bfloat16 [4096, 1024], P(None, 'tensor'), may hold values from -0.09375 to 0.09375
- out_weight: bfloat16 [8192, 4096], P('tensor'), may hold values from -0.0625 to 0.0625
- past_cache: bfloat16 [1024, 64, 2, 1024], P('dp', None, None, 'tensor'), parts along dimension 0, may hold values from -320 to 320
- exponents: int32 [10240, 32], P('dp'), parts along dimension 0, may hold values from -11 to -7
Outputs:
- mixed: bfloat16 [10240, 4096], P(('dp', 'tensor')), parts along dimension 0
The draws below stay inside these ranges and needn't reach their ends.
There are 8 independent parts, one for each index of `dp`. The reference program is written for one: setup_inputs(seed, part) draws one part's arguments, and reference() takes and returns one part's arrays. A program takes and returns all parts, laid end to end along the dimension named above; an argument that names none is the same for every part. Nothing has to cross between parts.
All inputs are finite; a program needn't handle non-finite values.
Results may differ from the reference program's by a relative error of at most 0.012.
The reference program's roundings to bfloat16 on the way count: a program that leaves them out, or rounds other values in their place, can miss the bound.
Values may be sent and summed in bfloat16 or wider, within the bound.
A program may use at most 192 MiB of HBM per device.

```python
import jax
import jax.numpy as jnp
from jax import lax

D = 4096
QH = 64
KVH = 8
HD = 128
SEQS = 128
NEW = 10
CACHE = 64
QG = 128
ROWS = 1280
N_TENSOR = 4


def draw_past_cache(key, part):
    key_base = jax.random.fold_in(key, 11)
    shape_full = (SEQS, CACHE, 2, KVH * HD)
    values_out = jnp.clip(jax.random.normal(key_base, shape_full, jnp.float32), -4.0, 4.0)
    return values_out.astype(jnp.bfloat16)


def with_ends(array, key, least, top_value):
    longest = array.shape.index(max(array.shape))
    spots = []
    for shift in (0, 1):
        where = [jax.random.randint(jax.random.fold_in(key, axis), (), 0, length) for axis, length in enumerate(array.shape)]
        where[longest] = (where[longest] + shift) % array.shape[longest]
        spots.append(tuple(where))
    return array.at[spots[0]].set(least).at[spots[1]].set(top_value)


def block_scale(rng, dims, pieces, smallest, high):
    def one(dim, blocks):
        draws = jax.random.uniform(jax.random.fold_in(jax.random.fold_in(rng, 6), dim), (blocks,), jnp.float32, smallest / len(pieces), high / len(pieces))
        return jnp.repeat(jnp.exp(draws), dims[dim] // blocks).reshape((-1,) + (1,) * (len(dims) - dim - 1))

    gain = one(*pieces[0])
    for cut in pieces[1:]:
        gain = gain * one(*cut)
    return gain


def scatter_about(own_key, shape, width, limit, pieces=(), kind=jnp.bfloat16):
    gain = block_scale(own_key, shape, pieces, -0.22, 0.18) if pieces else 1.0
    result = jax.random.normal(own_key, shape, jnp.float32) * width * gain
    return jnp.minimum(jnp.maximum(result, -limit), limit).astype(kind)


def setup_inputs(seed: int = 0, part: int = 0) -> dict:
    streams_of = jax.random.split(jax.random.key(seed), 9)
    own_keys = jax.random.split(jax.random.fold_in(streams_of[8], part), 9)
    return {
        "tokens": scatter_about(own_keys[0], (ROWS, D), 1.0, 6.0, ((0, 4),)),
        "norm_gain": jnp.clip(1.0 + 0.18 * jax.random.normal(streams_of[1], (D,), jnp.float32), 0.099609375, 1.8984375).astype(jnp.bfloat16),
        "query_weight": scatter_about(streams_of[2], (D, QH * HD), D ** -0.5, 0.09375, ((1, 4),)),
        "key_weight": scatter_about(streams_of[3], (D, KVH * HD), D ** -0.5, 0.09375, ((1, 4),)),
        "value_weight": scatter_about(streams_of[4], (D, KVH * HD), D ** -0.5, 0.09375, ((1, 4),)),
        "out_weight": scatter_about(streams_of[5], (QH * HD, D), (QH * HD) ** -0.5, 0.0625, ((0, 4),)),
        "past_cache": draw_past_cache(jax.random.fold_in(jax.random.fold_in(streams_of[8], part), 71), part),
        "exponents": with_ends(jax.random.randint(own_keys[7], (ROWS, D // QG), -11, -6), jax.random.fold_in(own_keys[7], 1), -11, (-6) - 1).astype(jnp.int32),
    }


epsilon = 1e-05
theta_base = 500000.0

def rotate(matrix, heads):
    row_count = matrix.shape[0]
    half_dim = HD // 2
    positions = (jnp.arange(row_count, dtype=jnp.int32) % NEW + CACHE).astype(jnp.float32)
    frequency = theta_base ** (-(jnp.arange(half_dim, dtype=jnp.float32) * 2.0) / HD)
    angles = positions[:, None] * frequency[None, :]
    cosine = jnp.cos(angles)[:, None, :]
    sine_part = jnp.sin(angles)[:, None, :]
    shaped = matrix.reshape(row_count, heads, 2, half_dim)
    first = shaped[:, :, 0]
    second = shaped[:, :, 1]
    turned = jnp.stack([first * cosine - second * sine_part, second * cosine + first * sine_part], 2)
    return turned.reshape(row_count, heads * HD)

def attention(query, key_new, value_new, past_cache, kv_heads):
    row_count = query.shape[0]
    seq_count = row_count // NEW
    group_size = query.shape[1] // (kv_heads * HD)
    cache_len = past_cache.shape[1]
    query_heads = query.astype(jnp.float32).reshape(seq_count, NEW, kv_heads, group_size, HD)
    new_keys = key_new.astype(jnp.float32).reshape(seq_count, NEW, kv_heads, HD)
    new_values = value_new.astype(jnp.float32).reshape(seq_count, NEW, kv_heads, HD)
    cache_keys = past_cache[:, :, 0].astype(jnp.float32).reshape(seq_count, cache_len, kv_heads, HD)
    cache_values = past_cache[:, :, 1].astype(jnp.float32).reshape(seq_count, cache_len, kv_heads, HD)
    inv_root = 1.0 / HD ** 0.5
    cache_scores = jnp.einsum('stkgd,sckd->skgtc', query_heads, cache_keys) * inv_root
    new_scores = jnp.einsum('stkgd,sukd->skgtu', query_heads, new_keys) * inv_root
    causal = jnp.arange(NEW)[:, None] >= jnp.arange(NEW)[None, :]
    new_scores = jnp.where(causal, new_scores, -1e+30)
    row_max = jnp.maximum(cache_scores.max(-1), new_scores.max(-1))[..., None]
    cache_probs = jnp.exp(cache_scores - row_max)
    new_probs = jnp.exp(new_scores - row_max)
    denominator = (cache_probs.sum(-1) + new_probs.sum(-1))[..., None]
    cache_weights = (cache_probs / denominator).astype(jnp.bfloat16).astype(jnp.float32)
    new_weights = (new_probs / denominator).astype(jnp.bfloat16).astype(jnp.float32)
    combined = jnp.einsum('skgtc,sckd->stkgd', cache_weights, cache_values)
    combined = combined + jnp.einsum('skgtu,sukd->stkgd', new_weights, new_values)
    return combined.reshape(row_count, kv_heads * group_size * HD).astype(jnp.bfloat16)

def reference(tokens, norm_gain, query_weight, key_weight, value_weight, out_weight, past_cache, exponents):
    floats = tokens.astype(jnp.float32)
    normed = floats * lax.rsqrt(lax.optimization_barrier(jnp.mean(floats * floats, axis=-1, keepdims=True)) + epsilon)
    normed = (normed * norm_gain.astype(jnp.float32)).astype(jnp.bfloat16)
    query = rotate(jnp.dot(normed, query_weight, preferred_element_type=jnp.float32), QH).astype(jnp.bfloat16)
    key_new = rotate(jnp.dot(normed, key_weight, preferred_element_type=jnp.float32), KVH).astype(jnp.bfloat16)
    value_new = jnp.dot(normed, value_weight, preferred_element_type=jnp.float32).astype(jnp.bfloat16)
    attended = attention(query, key_new, value_new, past_cache, KVH)
    row_count = tokens.shape[0]
    groups = D // QG
    shrink = jnp.exp2(-exponents.astype(jnp.float32))[..., None]
    head_cols = QH * HD // N_TENSOR
    summed = jnp.zeros((row_count, groups, QG), jnp.float32)
    for rank in range(N_TENSOR):
        partial_value = jnp.dot(attended[:, rank * head_cols:(rank + 1) * head_cols], out_weight[rank * head_cols:(rank + 1) * head_cols], preferred_element_type=jnp.float32)
        scaled = jnp.clip(partial_value.reshape(row_count, groups, QG) * shrink, -127.0, 127.0)
        summed = summed + lax.optimization_barrier(scaled.astype(jnp.bfloat16)).astype(jnp.float32)
    restore = jnp.exp2(exponents.astype(jnp.float32))[..., None]
    layer_out = floats + (summed * restore).reshape(row_count, D)
    return layer_out.astype(jnp.bfloat16)
```

```python
import functools

import jax
import jax.numpy as jnp
from jax import lax
from jax.experimental import pallas as pl
from jax.experimental.pallas import tpu as pltpu
from jax.sharding import PartitionSpec as P

HD = 128
NEW = 10
CHUNKS = 2
SEQ_BLOCK = 8

epsilon = 1e-05
theta_base = 500000.0


def rotary_tables(row_count):
    half_dim = HD // 2
    positions = (jnp.arange(row_count, dtype=jnp.int32) % NEW + 64).astype(jnp.float32)
    frequency = theta_base ** (-(jnp.arange(half_dim, dtype=jnp.float32) * 2.0) / HD)
    angles = positions[:, None] * frequency[None, :]
    cosine = jnp.cos(angles)
    sine_part = jnp.sin(angles)
    return (
        jnp.concatenate([cosine, cosine], 1),
        jnp.concatenate([-sine_part, sine_part], 1),
    )


def turn(block, cosine, sine_part):
    heads = []
    for h in range(block.shape[1] // HD):
        head = block[:, h * HD : (h + 1) * HD]
        heads.append(head * cosine + pltpu.roll(head, HD // 2, 1) * sine_part)
    return jnp.concatenate(heads, 1) if len(heads) > 1 else heads[0]


def project_kernel(x_ref, wq_ref, wk_ref, wv_ref, cos_ref, sin_ref, q_ref, k_ref, v_ref):
    normed = x_ref[...]
    cosine = cos_ref[...]
    sine_part = sin_ref[...]

    @pl.when(pl.program_id(0) == 0)
    def _():
        key = jnp.dot(normed, wk_ref[...], preferred_element_type=jnp.float32)
        k_ref[...] = turn(key, cosine, sine_part).astype(jnp.bfloat16)
        value = jnp.dot(normed, wv_ref[...], preferred_element_type=jnp.float32)
        v_ref[...] = value.astype(jnp.bfloat16)

    query = jnp.dot(normed, wq_ref[...], preferred_element_type=jnp.float32)
    q_ref[...] = turn(query, cosine, sine_part).astype(jnp.bfloat16)


def project(normed, query_weight, key_weight, value_weight, cosine, sine_part):
    rows, depth = normed.shape
    q_cols = query_weight.shape[1]
    k_cols = key_weight.shape[1]
    width = 512
    whole = lambda j: (0, 0)
    return pl.pallas_call(
        project_kernel,
        grid=(q_cols // width,),
        in_specs=[
            pl.BlockSpec((rows, depth), whole),
            pl.BlockSpec((depth, width), lambda j: (0, j)),
            pl.BlockSpec((depth, k_cols), whole),
            pl.BlockSpec((depth, k_cols), whole),
            pl.BlockSpec((rows, HD), whole),
            pl.BlockSpec((rows, HD), whole),
        ],
        out_specs=[
            pl.BlockSpec((rows, width), lambda j: (0, j)),
            pl.BlockSpec((rows, k_cols), whole),
            pl.BlockSpec((rows, k_cols), whole),
        ],
        out_shape=[
            jax.ShapeDtypeStruct((rows, q_cols), jnp.bfloat16),
            jax.ShapeDtypeStruct((rows, k_cols), jnp.bfloat16),
            jax.ShapeDtypeStruct((rows, k_cols), jnp.bfloat16),
        ],
        compiler_params=pltpu.CompilerParams(vmem_limit_bytes=56 * 1024 * 1024),
    )(normed, query_weight, key_weight, value_weight, cosine, sine_part)


def attend_kernel(kv_heads, group, q_ref, k_ref, v_ref, cache_ref, bias_ref, out_ref):
    rows = q_ref.shape[0]
    inv_root = 1.0 / HD**0.5
    bias = bias_ref[...]
    for kv in range(kv_heads):
        base = kv * group * HD
        query = jnp.concatenate(
            [q_ref[:, base + g * HD : base + (g + 1) * HD] for g in range(group)], 0
        )
        span = slice(kv * HD, (kv + 1) * HD)
        v_span = slice((kv_heads + kv) * HD, (kv_heads + kv + 1) * HD)
        keys = jnp.concatenate([cache_ref[:, span], k_ref[:, span]], 0)
        values = jnp.concatenate([cache_ref[:, v_span], v_ref[:, span]], 0)
        scores = lax.dot_general(
            query, keys, (((1,), (1,)), ((), ())), preferred_element_type=jnp.float32
        )
        weights = []
        for g in range(group):
            part = scores[g * rows : (g + 1) * rows] * inv_root + bias
            probs = jnp.exp(part - jnp.max(part, axis=-1, keepdims=True))
            scale = 1.0 / jnp.sum(probs, axis=-1, keepdims=True)
            weights.append((probs * scale).astype(jnp.bfloat16))
        combined = jnp.dot(
            jnp.concatenate(weights, 0), values, preferred_element_type=jnp.float32
        ).astype(jnp.bfloat16)
        for g in range(group):
            out_ref[:, base + g * HD : base + (g + 1) * HD] = combined[
                g * rows : (g + 1) * rows
            ]


def attend(query, key_new, value_new, cache, cache_len, ranks, chunk):
    rows, q_cols = query.shape
    k_cols = key_new.shape[1]
    kv_heads = k_cols // HD
    group = q_cols // k_cols
    block_rows = SEQ_BLOCK * NEW
    blocks = rows // block_rows
    per_rank = blocks // ranks
    cache_rows = SEQ_BLOCK * cache_len
    row_seq = jnp.arange(block_rows)[:, None] // NEW
    row_new = jnp.arange(block_rows)[:, None] % NEW
    in_cache = row_seq == jnp.arange(cache_rows)[None, :] // cache_len
    new_col = jnp.arange(block_rows)[None, :]
    in_new = (row_seq == new_col // NEW) & (row_new >= new_col % NEW)
    bias = jnp.where(jnp.concatenate([in_cache, in_new], 1), 0.0, -1e30).astype(jnp.float32)
    return pl.pallas_call(
        functools.partial(attend_kernel, kv_heads, group),
        grid=(blocks,),
        in_specs=[
            pl.BlockSpec((block_rows, q_cols), lambda i: (i, 0)),
            pl.BlockSpec((block_rows, k_cols), lambda i: (i, 0)),
            pl.BlockSpec((block_rows, k_cols), lambda i: (i, 0)),
            pl.BlockSpec(
                (cache_rows, 2 * k_cols),
                lambda i: (
                    (i // per_rank) * (per_rank * CHUNKS) + chunk * per_rank + i % per_rank,
                    0,
                ),
            ),
            pl.BlockSpec((block_rows, cache_rows + block_rows), lambda i: (0, 0)),
        ],
        out_specs=pl.BlockSpec((block_rows, q_cols), lambda i: (i, 0)),
        out_shape=jax.ShapeDtypeStruct((rows, q_cols), jnp.bfloat16),
        compiler_params=pltpu.CompilerParams(vmem_limit_bytes=56 * 1024 * 1024),
    )(query, key_new, value_new, cache, bias)


def out_kernel(group_cols, a_ref, w_ref, shrink_ref, out_ref):
    partial_value = jnp.dot(a_ref[...], w_ref[...], preferred_element_type=jnp.float32)
    for i in range(out_ref.shape[1] // group_cols):
        span = slice(i * group_cols, (i + 1) * group_cols)
        scaled = jnp.clip(partial_value[:, span] * shrink_ref[0, :, i : i + 1], -127.0, 127.0)
        out_ref[:, span] = scaled.astype(jnp.bfloat16)


def project_out(attended, out_weight, shrink):
    rows, depth = attended.shape
    cols = out_weight.shape[1]
    groups = shrink.shape[1]
    group_cols = cols // groups
    width = 512
    per_block = width // group_cols
    shrink = shrink.reshape(rows, groups // per_block, per_block).transpose(1, 0, 2)
    return pl.pallas_call(
        functools.partial(out_kernel, group_cols),
        grid=(cols // width,),
        in_specs=[
            pl.BlockSpec((rows, depth), lambda j: (0, 0)),
            pl.BlockSpec((depth, width), lambda j: (0, j)),
            pl.BlockSpec((1, rows, per_block), lambda j: (j, 0, 0)),
        ],
        out_specs=pl.BlockSpec((rows, width), lambda j: (0, j)),
        out_shape=jax.ShapeDtypeStruct((rows, cols), jnp.bfloat16),
        compiler_params=pltpu.CompilerParams(vmem_limit_bytes=56 * 1024 * 1024),
    )(attended, out_weight, shrink)


def on_device(
    tokens, norm_gain, query_weight, key_weight, value_weight, out_weight, past_cache, exponents
):
    own_rows, depth = tokens.shape
    ranks = lax.axis_size("tensor")
    step = own_rows // CHUNKS
    groups = exponents.shape[1]
    cache_len = past_cache.shape[1]
    gain_f32 = norm_gain.astype(jnp.float32)
    floats = tokens.astype(jnp.float32)
    gathered = []
    for c in range(CHUNKS):
        piece = floats[c * step : (c + 1) * step]
        normed = piece * lax.rsqrt(jnp.mean(piece * piece, axis=-1, keepdims=True) + epsilon)
        normed = (normed * gain_f32).astype(jnp.bfloat16)
        gathered.append(lax.all_gather(normed, "tensor", axis=0, tiled=True))
    cache = past_cache.reshape(past_cache.shape[0] * cache_len, -1)
    cosine, sine_part = rotary_tables(step * ranks)
    shrink = jnp.exp2(-exponents.astype(jnp.float32)).reshape(ranks, CHUNKS, step, groups)
    shares = []
    for c in range(CHUNKS):
        query, key_new, value_new = project(
            gathered[c], query_weight, key_weight, value_weight, cosine, sine_part
        )
        attended = attend(query, key_new, value_new, cache, cache_len, ranks, c)
        rounded = project_out(
            attended, out_weight, shrink[:, c].reshape(ranks * step, groups)
        )
        shares.append(lax.psum_scatter(rounded, "tensor", scatter_dimension=0, tiled=True))
    own_exponents = lax.dynamic_slice_in_dim(
        exponents, lax.axis_index("tensor") * own_rows, own_rows, 0
    )
    restore = jnp.exp2(own_exponents.astype(jnp.float32))
    outs = []
    for c in range(CHUNKS):
        span = slice(c * step, (c + 1) * step)
        wide = jnp.repeat(restore[span], depth // groups, axis=1)
        outs.append((floats[span] + shares[c].astype(jnp.float32) * wide).astype(jnp.bfloat16))
    return jnp.concatenate(outs, 0)


def solution(mesh):
    return jax.shard_map(
        on_device,
        mesh=mesh,
        in_specs=(
            P(("dp", "tensor"), None),
            P(),
            P(None, "tensor"),
            P(None, "tensor"),
            P(None, "tensor"),
            P("tensor", None),
            P("dp", None, None, "tensor"),
            P("dp", None),
        ),
        out_specs=P(("dp", "tensor"), None),
        check_vma=False,
    )
```

```python
import functools

import jax
import jax.numpy as jnp
from jax import lax
from jax.experimental import pallas as pl
from jax.experimental.pallas import tpu as pltpu
from jax.sharding import PartitionSpec as P

HD = 128
NEW = 10
CHUNKS = 2
SEQ_BLOCK = 8

epsilon = 1e-05
theta_base = 500000.0


def rotary_tables(row_count):
    half_dim = HD // 2
    positions = (jnp.arange(row_count, dtype=jnp.int32) % NEW + 64).astype(jnp.float32)
    frequency = theta_base ** (-(jnp.arange(half_dim, dtype=jnp.float32) * 2.0) / HD)
    angles = positions[:, None] * frequency[None, :]
    cosine = jnp.cos(angles)
    sine_part = jnp.sin(angles)
    return (
        jnp.concatenate([cosine, cosine], 1),
        jnp.concatenate([-sine_part, sine_part], 1),
    )


def turn(block, cosine, sine_part):
    heads = []
    for h in range(block.shape[1] // HD):
        head = block[:, h * HD : (h + 1) * HD]
        heads.append(head * cosine + pltpu.roll(head, HD // 2, 1) * sine_part)
    return jnp.concatenate(heads, 1) if len(heads) > 1 else heads[0]


def project_kernel(x_ref, wq_ref, wk_ref, wv_ref, cos_ref, sin_ref, q_ref, k_ref, v_ref):
    normed = x_ref[...]
    cosine = cos_ref[...]
    sine_part = sin_ref[...]

    @pl.when(pl.program_id(0) == 0)
    def _():
        key = jnp.dot(normed, wk_ref[...], preferred_element_type=jnp.float32)
        k_ref[...] = turn(key, cosine, sine_part).astype(jnp.bfloat16)
        value = jnp.dot(normed, wv_ref[...], preferred_element_type=jnp.float32)
        v_ref[...] = value.astype(jnp.bfloat16)

    query = jnp.dot(normed, wq_ref[...], preferred_element_type=jnp.float32)
    q_ref[...] = turn(query, cosine, sine_part).astype(jnp.bfloat16)


def project(normed, query_weight, key_weight, value_weight, cosine, sine_part):
    rows, depth = normed.shape
    q_cols = query_weight.shape[1]
    k_cols = key_weight.shape[1]
    width = 512
    whole = lambda j: (0, 0)
    return pl.pallas_call(
        project_kernel,
        grid=(q_cols // width,),
        in_specs=[
            pl.BlockSpec((rows, depth), whole),
            pl.BlockSpec((depth, width), lambda j: (0, j)),
            pl.BlockSpec((depth, k_cols), whole),
            pl.BlockSpec((depth, k_cols), whole),
            pl.BlockSpec((rows, HD), whole),
            pl.BlockSpec((rows, HD), whole),
        ],
        out_specs=[
            pl.BlockSpec((rows, width), lambda j: (0, j)),
            pl.BlockSpec((rows, k_cols), whole),
            pl.BlockSpec((rows, k_cols), whole),
        ],
        out_shape=[
            jax.ShapeDtypeStruct((rows, q_cols), jnp.bfloat16),
            jax.ShapeDtypeStruct((rows, k_cols), jnp.bfloat16),
            jax.ShapeDtypeStruct((rows, k_cols), jnp.bfloat16),
        ],
        compiler_params=pltpu.CompilerParams(vmem_limit_bytes=56 * 1024 * 1024),
    )(normed, query_weight, key_weight, value_weight, cosine, sine_part)


def attend_kernel(kv_heads, group, q_ref, k_ref, v_ref, cache_ref, bias_ref, out_ref):
    rows = q_ref.shape[0]
    inv_root = 1.0 / HD**0.5
    bias = bias_ref[...]
    for kv in range(kv_heads):
        base = kv * group * HD
        query = jnp.concatenate(
            [q_ref[:, base + g * HD : base + (g + 1) * HD] for g in range(group)], 0
        )
        span = slice(kv * HD, (kv + 1) * HD)
        v_span = slice((kv_heads + kv) * HD, (kv_heads + kv + 1) * HD)
        keys = jnp.concatenate([cache_ref[:, span], k_ref[:, span]], 0)
        values = jnp.concatenate([cache_ref[:, v_span], v_ref[:, span]], 0)
        scores = lax.dot_general(
            query, keys, (((1,), (1,)), ((), ())), preferred_element_type=jnp.float32
        )
        weights = []
        for g in range(group):
            part = scores[g * rows : (g + 1) * rows] * inv_root + bias
            probs = jnp.exp(part - jnp.max(part, axis=-1, keepdims=True))
            scale = 1.0 / jnp.sum(probs, axis=-1, keepdims=True)
            weights.append((probs * scale).astype(jnp.bfloat16))
        combined = jnp.dot(
            jnp.concatenate(weights, 0), values, preferred_element_type=jnp.float32
        ).astype(jnp.bfloat16)
        for g in range(group):
            out_ref[:, base + g * HD : base + (g + 1) * HD] = combined[
                g * rows : (g + 1) * rows
            ]


def attend(query, key_new, value_new, cache, cache_len, ranks, chunk):
    rows, q_cols = query.shape
    k_cols = key_new.shape[1]
    kv_heads = k_cols // HD
    group = q_cols // k_cols
    block_rows = SEQ_BLOCK * NEW
    blocks = rows // block_rows
    per_rank = blocks // ranks
    cache_rows = SEQ_BLOCK * cache_len
    row_seq = jnp.arange(block_rows)[:, None] // NEW
    row_new = jnp.arange(block_rows)[:, None] % NEW
    in_cache = row_seq == jnp.arange(cache_rows)[None, :] // cache_len
    new_col = jnp.arange(block_rows)[None, :]
    in_new = (row_seq == new_col // NEW) & (row_new >= new_col % NEW)
    bias = jnp.where(jnp.concatenate([in_cache, in_new], 1), 0.0, -1e30).astype(jnp.float32)
    return pl.pallas_call(
        functools.partial(attend_kernel, kv_heads, group),
        grid=(blocks,),
        in_specs=[
            pl.BlockSpec((block_rows, q_cols), lambda i: (i, 0)),
            pl.BlockSpec((block_rows, k_cols), lambda i: (i, 0)),
            pl.BlockSpec((block_rows, k_cols), lambda i: (i, 0)),
            pl.BlockSpec(
                (cache_rows, 2 * k_cols),
                lambda i: (
                    (i // per_rank) * (per_rank * CHUNKS) + chunk * per_rank + i % per_rank,
                    0,
                ),
            ),
            pl.BlockSpec((block_rows, cache_rows + block_rows), lambda i: (0, 0)),
        ],
        out_specs=pl.BlockSpec((block_rows, q_cols), lambda i: (i, 0)),
        out_shape=jax.ShapeDtypeStruct((rows, q_cols), jnp.bfloat16),
        compiler_params=pltpu.CompilerParams(vmem_limit_bytes=56 * 1024 * 1024),
    )(query, key_new, value_new, cache, bias)


def out_kernel(group_cols, a_ref, w_ref, shrink_ref, out_ref):
    partial_value = jnp.dot(a_ref[...], w_ref[...], preferred_element_type=jnp.float32)
    for i in range(out_ref.shape[1] // group_cols):
        span = slice(i * group_cols, (i + 1) * group_cols)
        scaled = jnp.clip(partial_value[:, span] * shrink_ref[0, :, i : i + 1], -127.0, 127.0)
        out_ref[:, span] = scaled.astype(jnp.bfloat16)


def project_out(attended, out_weight, shrink):
    rows, depth = attended.shape
    cols = out_weight.shape[1]
    groups = shrink.shape[1]
    group_cols = cols // groups
    width = 512
    per_block = width // group_cols
    shrink = shrink.reshape(rows, groups // per_block, per_block).transpose(1, 0, 2)
    return pl.pallas_call(
        functools.partial(out_kernel, group_cols),
        grid=(cols // width,),
        in_specs=[
            pl.BlockSpec((rows, depth), lambda j: (0, 0)),
            pl.BlockSpec((depth, width), lambda j: (0, j)),
            pl.BlockSpec((1, rows, per_block), lambda j: (j, 0, 0)),
        ],
        out_specs=pl.BlockSpec((rows, width), lambda j: (0, j)),
        out_shape=jax.ShapeDtypeStruct((rows, cols), jnp.bfloat16),
        compiler_params=pltpu.CompilerParams(vmem_limit_bytes=56 * 1024 * 1024),
    )(attended, out_weight, shrink)


def norm_kernel(x_ref, gain_ref, out_ref):
    floats = x_ref[...].astype(jnp.float32)
    normed = floats * lax.rsqrt(jnp.mean(floats * floats, axis=-1, keepdims=True) + epsilon)
    out_ref[...] = (normed * gain_ref[...].astype(jnp.float32)).astype(jnp.bfloat16)


def normalise(tokens, gain, step, chunk):
    depth = tokens.shape[1]
    return pl.pallas_call(
        norm_kernel,
        grid=(1,),
        in_specs=[
            pl.BlockSpec((step, depth), lambda i: (chunk, 0)),
            pl.BlockSpec((1, depth), lambda i: (0, 0)),
        ],
        out_specs=pl.BlockSpec((step, depth), lambda i: (0, 0)),
        out_shape=jax.ShapeDtypeStruct((step, depth), jnp.bfloat16),
    )(tokens, gain)


def residual_kernel(tokens_ref, restore_ref, *refs):
    out_ref = refs[-1]
    start = 0
    groups = restore_ref.shape[1]
    width = tokens_ref.shape[1] // groups
    for share_ref in refs[:-1]:
        rows = slice(start, start + share_ref.shape[0])
        start += share_ref.shape[0]
        for g in range(groups):
            cols = slice(g * width, (g + 1) * width)
            term = share_ref[:, cols].astype(jnp.float32) * restore_ref[rows, g : g + 1]
            out_ref[rows, cols] = (tokens_ref[rows, cols].astype(jnp.float32) + term).astype(
                jnp.bfloat16
            )


def add_residual(tokens, shares, restore):
    return pl.pallas_call(
        residual_kernel,
        out_shape=jax.ShapeDtypeStruct(tokens.shape, jnp.bfloat16),
    )(tokens, restore, *shares)


def on_device(
    tokens, norm_gain, query_weight, key_weight, value_weight, out_weight, past_cache, exponents
):
    own_rows, depth = tokens.shape
    ranks = lax.axis_size("tensor")
    step = own_rows // CHUNKS
    groups = exponents.shape[1]
    cache_len = past_cache.shape[1]
    gathered = []
    for c in range(CHUNKS):
        normed = normalise(tokens, norm_gain.reshape(1, depth), step, c)
        gathered.append(lax.all_gather(normed, "tensor", axis=0, tiled=True))
    cache = past_cache.reshape(past_cache.shape[0] * cache_len, -1)
    cosine, sine_part = rotary_tables(step * ranks)
    shrink = jnp.exp2(-exponents.astype(jnp.float32)).reshape(ranks, CHUNKS, step, groups)
    shares = []
    for c in range(CHUNKS):
        query, key_new, value_new = project(
            gathered[c], query_weight, key_weight, value_weight, cosine, sine_part
        )
        attended = attend(query, key_new, value_new, cache, cache_len, ranks, c)
        rounded = project_out(
            attended, out_weight, shrink[:, c].reshape(ranks * step, groups)
        )
        shares.append(lax.psum_scatter(rounded, "tensor", scatter_dimension=0, tiled=True))
    own_exponents = lax.dynamic_slice_in_dim(
        exponents, lax.axis_index("tensor") * own_rows, own_rows, 0
    )
    restore = jnp.exp2(own_exponents.astype(jnp.float32))
    return add_residual(tokens, shares, restore)


def solution(mesh):
    return jax.shard_map(
        on_device,
        mesh=mesh,
        in_specs=(
            P(("dp", "tensor"), None),
            P(),
            P(None, "tensor"),
            P(None, "tensor"),
            P(None, "tensor"),
            P("tensor", None),
            P("dp", None, None, "tensor"),
            P("dp", None),
        ),
        out_specs=P(("dp", "tensor"), None),
        check_vma=False,
    )
```
